256 devices in a mesh: dp: 32 (over x, z_lo, core), head: 8 (over y, z_hi).
Axes of the slice: x: 4, y: 4, z: 8 (z_hi: 2, z_lo: 4; z = z_hi * 4 + z_lo), core: 2. Of those that a mesh axis runs over, the one named last changes fastest.
Arguments:
- frames_in: bfloat16 [32, 8, 320, 640], P('dp', 'head'), may hold values from -6 to 6
- ln1_gain: float32 [1280], replicated, may hold values from 0.25 to 1.75
- ln1_bias: float32 [1280], replicated, may hold values from -3 to 3
- qkv_weight: bfloat16 [1280, 3, 1024], P('dp', None, 'head'), may hold values from -0.1875 to 0.1875
- qv_bias: float32 [2, 1024], P(None, 'head'), may hold values from -3 to 3
- out_weight: bfloat16 [1024, 1280], P(('head', 'dp')), may hold values from -0.1875 to 0.1875
- out_bias: float32 [1280], P('head'), may hold values from -3 to 3
- ln2_gain: float32 [1280], replicated, may hold values from 0.25 to 1.75
- ln2_bias: float32 [1280], replicated, may hold values from -3 to 3
- fc1_weight: bfloat16 [1280, 5120], P('dp', 'head'), may hold values from -0.15625 to 0.15625
- fc1_bias: float32 [5120], P('head'), may hold values from -3 to 3
- fc2_weight: bfloat16 [5120, 1280], P(('head', 'dp')), may hold values from -0.078125 to 0.078125
- fc2_bias: float32 [1280], P('head'), may hold values from -3 to 3
- server_of_clip: int32 [32], replicated, may hold values from 0 to 7
Outputs:
- encoded: bfloat16 [32, 8, 320, 640], P('dp', 'head')
The draws below stay inside these ranges and needn't reach their ends.
All inputs are finite; a program needn't handle non-finite values.
Results may differ from the reference program's by a relative error of at most 0.014.
Values may be sent and summed in bfloat16 or wider, within the bound.
No kernel may reach another device: no remote copies, remote signals or barrier semaphores. Data moves between devices by JAX's collectives and lax.ppermute only.
A program may use at most 64 MiB of HBM per device.

```python
import jax
import jax.numpy as jnp
from jax import lax

D = 1280
HEADS = 16
HDIM = 64
MLP = 5120
FRAMES = 1280
SERVERS = 8
CLIPS = 32
N_HEAD = 8


def draw_qkv_weight(key, part):
    normal = jax.random.normal(jax.random.fold_in(key, 29), (D, 3, HEADS * HDIM), jnp.float32)
    return jnp.clip(normal * D ** (-0.5), -0.1875, 0.1875).astype(jnp.bfloat16)


def plant(entries, own_key, low, high):
    index_at = [jax.random.randint(jax.random.fold_in(own_key, axis), (), 0, length) for axis, length in enumerate(entries.shape)]
    widest = entries.shape.index(max(entries.shape))
    next_to = index_at[:widest] + [(index_at[widest] + 1) % entries.shape[widest]] + index_at[widest + 1:]
    return entries.at[tuple(index_at)].set(low).at[tuple(next_to)].set(high)


def block_levels(own_key, extent, split, low, top_value):
    level, own = 1.0, jax.random.fold_in(own_key, 6)
    for axis_at, shards_of in split:
        heights = jnp.exp(jax.random.uniform(jax.random.fold_in(own, axis_at), (shards_of,), jnp.float32, low / len(split), top_value / len(split)))
        level = level * jnp.repeat(heights, extent[axis_at] // shards_of).reshape([-1 if axis == axis_at else 1 for axis in range(len(extent))])
    return level


def noise(own_key, extent, deviation, most, split=(), held_as=jnp.bfloat16):
    level = block_levels(own_key, extent, split, -0.22, 0.18) if split else 1.0
    values = jax.random.normal(own_key, extent, jnp.float32) * deviation * level
    return jnp.minimum(jnp.maximum(values, -most), most).astype(held_as)


def setup_inputs(seed: int = 0) -> dict:
    streams_of = jax.random.split(jax.random.key(seed), 15)
    return {
        "frames_in": noise(streams_of[0], (CLIPS, N_HEAD, FRAMES // 4, 4 * D // N_HEAD), 1.0, 6.0, ((0, 32), (1, 8))),
        "ln1_gain": jnp.clip(1.0 + 0.15 * jax.random.normal(streams_of[1], (D,), jnp.float32), 0.25, 1.75),
        "ln1_bias": noise(streams_of[2], (D,), 0.5, 3.0, (), jnp.float32),
        "qkv_weight": draw_qkv_weight(jax.random.fold_in(streams_of[14], 71), 0),
        "qv_bias": noise(streams_of[4], (2, HEADS * HDIM), 0.5, 3.0, ((1, 8),), jnp.float32),
        "out_weight": noise(streams_of[5], (HEADS * HDIM, D), (HEADS * HDIM) ** -0.5, 0.1875, ((0, 256),)),
        "out_bias": noise(streams_of[6], (D,), 0.5, 3.0, ((0, 8),), jnp.float32),
        "ln2_gain": jnp.clip(1.0 + 0.15 * jax.random.normal(streams_of[7], (D,), jnp.float32), 0.25, 1.75),
        "ln2_bias": noise(streams_of[8], (D,), 0.5, 3.0, (), jnp.float32),
        "fc1_weight": noise(streams_of[9], (D, MLP), D ** -0.5, 0.15625, ((0, 32), (1, 8))),
        "fc1_bias": noise(streams_of[10], (MLP,), 0.5, 3.0, ((0, 8),), jnp.float32),
        "fc2_weight": noise(streams_of[11], (MLP, D), MLP ** -0.5, 0.078125, ((0, 256),)),
        "fc2_bias": noise(streams_of[12], (D,), 0.5, 3.0, ((0, 8),), jnp.float32),
        "server_of_clip": plant(jax.random.randint(streams_of[13], (CLIPS,), 0, SERVERS), jax.random.fold_in(streams_of[13], 1), 0, SERVERS - 1).astype(jnp.int32),
    }


epsilon = 1e-05

def layer_norm(matrix, gain_row, shift_row):
    floats = matrix.astype(jnp.float32)
    center = lax.optimization_barrier(jnp.mean(floats, axis=-1, keepdims=True))
    spread = lax.optimization_barrier(jnp.mean(jnp.square(floats - center), axis=-1, keepdims=True))
    return ((floats - center) * lax.rsqrt(spread + epsilon) * gain_row + shift_row).astype(jnp.bfloat16)

def attend(queries, key_rows, value_rows):

    def single(triple):
        query_head, key_head, value_head = triple
        scores = jnp.dot(query_head, key_head.T, preferred_element_type=jnp.float32)
        maxima = lax.optimization_barrier(jnp.max(scores, axis=-1, keepdims=True))
        weights = jnp.exp(scores - maxima)
        probability = (weights / lax.optimization_barrier(jnp.sum(weights, axis=-1, keepdims=True))).astype(jnp.bfloat16)
        return jnp.dot(probability, value_head, preferred_element_type=jnp.float32).astype(jnp.bfloat16)
    per_head = lax.map(single, (jnp.swapaxes(queries, 0, 1), jnp.swapaxes(key_rows, 0, 1), jnp.swapaxes(value_rows, 0, 1)))
    return jnp.swapaxes(per_head, 0, 1).reshape(queries.shape[0], -1)

def slot_order(server_list):
    clip_count = server_list.shape[0]
    indices = jnp.arange(clip_count, dtype=jnp.int32)
    earlier = (server_list[None, :] < server_list[:, None]) | (server_list[None, :] == server_list[:, None]) & (indices[None, :] < indices[:, None])
    slot_of = lax.optimization_barrier(jnp.sum(earlier.astype(jnp.int32), axis=1)).astype(jnp.int32)
    return lax.optimization_barrier(jnp.sum(jnp.where(slot_of[None, :] == indices[:, None], indices[None, :], 0), axis=1)).astype(jnp.int32)

def reference(frames_in, ln1_gain, ln1_bias, qkv_weight, qv_bias, out_weight, out_bias, ln2_gain, ln2_bias, fc1_weight, fc1_bias, fc2_weight, fc2_bias, server_of_clip):
    block_width = D // N_HEAD
    clip_total = frames_in.shape[0]
    residual_all = frames_in.reshape(clip_total, N_HEAD, FRAMES // 4, 4, block_width).transpose(0, 2, 3, 1, 4).reshape(clip_total, FRAMES, D)

    def clip_layer(residual_in):
        frame_count = residual_in.shape[0]
        normed_one = layer_norm(residual_in, ln1_gain, ln1_bias)
        column_count = qkv_weight.shape[2]
        projected = jnp.dot(normed_one, qkv_weight.reshape(qkv_weight.shape[0], 3 * column_count), preferred_element_type=jnp.float32).reshape(frame_count, 3, column_count)
        queries = ((projected[:, 0] + qv_bias[0]) * HDIM ** (-0.5)).astype(jnp.bfloat16).reshape(frame_count, -1, HDIM)
        key_rows = projected[:, 1].astype(jnp.bfloat16).reshape(frame_count, -1, HDIM)
        value_rows = (projected[:, 2] + qv_bias[1]).astype(jnp.bfloat16).reshape(frame_count, -1, HDIM)
        context = attend(queries, key_rows, value_rows)
        attended = (residual_in.astype(jnp.float32) + out_bias + jnp.dot(context, out_weight, preferred_element_type=jnp.float32)).astype(jnp.bfloat16)
        normed_two = layer_norm(attended, ln2_gain, ln2_bias)
        hidden = jax.nn.gelu(jnp.dot(normed_two, fc1_weight, preferred_element_type=jnp.float32) + fc1_bias, approximate=False).astype(jnp.bfloat16)
        return (attended.astype(jnp.float32) + fc2_bias + jnp.dot(hidden, fc2_weight, preferred_element_type=jnp.float32)).astype(jnp.bfloat16)
    layer_out = lax.map(clip_layer, residual_all)
    clip_order = slot_order(server_of_clip)
    ordered = jnp.take(layer_out, clip_order, axis=0)
    return ordered.reshape(clip_total, FRAMES // 4, 4, N_HEAD, block_width).transpose(0, 3, 1, 2, 4).reshape(clip_total, N_HEAD, FRAMES // 4, 4 * block_width)
```

```python
import jax
import jax.numpy as jnp
from jax import lax
from jax.sharding import Mesh
from jax.sharding import PartitionSpec as P

HDIM = 64
DP = ("x", "zl", "core")
HEAD = ("y", "zh")
EPS = 1e-05


def exchange(value, axes):
    return lax.all_to_all(value, axes, split_axis=0, concat_axis=0, tiled=True)


def gather_y(value):
    copies = jnp.broadcast_to(value[None], (4, *value.shape))
    return exchange(copies, "y").reshape(4 * value.shape[0], value.shape[1])


def norm_columns(matrix, gain, shift):
    floats = matrix.astype(jnp.float32)
    center = jnp.mean(floats, axis=0, keepdims=True)
    spread = jnp.mean(jnp.square(floats - center), axis=0, keepdims=True)
    return ((floats - center) * lax.rsqrt(spread + EPS) * gain[:, None] + shift[:, None]).astype(
        jnp.bfloat16
    )


def dot_rows(left, right):
    return lax.dot_general(
        left, right, (((0,), (0,)), ((), ())), preferred_element_type=jnp.float32
    )


def slot_order(server_list):
    clip_count = server_list.shape[0]
    indices = jnp.arange(clip_count, dtype=jnp.int32)
    earlier = (server_list[None, :] < server_list[:, None]) | (
        server_list[None, :] == server_list[:, None]
    ) & (indices[None, :] < indices[:, None])
    slot_of = jnp.sum(earlier.astype(jnp.int32), axis=1)
    return jnp.sum(jnp.where(slot_of[None, :] == indices[:, None], indices[None, :], 0), axis=1)


def attend(queries, key_rows, value_rows):
    outs = []
    for at in range(0, queries.shape[0], HDIM):
        scores = dot_rows(key_rows[at : at + HDIM], queries[at : at + HDIM])
        maxima = jnp.max(scores, axis=0, keepdims=True)
        weights = jnp.exp(scores - maxima)
        probs = (weights / jnp.sum(weights, axis=0, keepdims=True)).astype(jnp.bfloat16)
        outs.append(
            jnp.dot(
                value_rows[at : at + HDIM], probs, preferred_element_type=jnp.float32
            ).astype(jnp.bfloat16)
        )
    return jnp.concatenate(outs, axis=0)


def on_device(
    frames_in,
    ln1_gain,
    ln1_bias,
    qkv_weight,
    qv_bias,
    out_weight,
    out_bias,
    ln2_gain,
    ln2_bias,
    fc1_weight,
    fc1_bias,
    fc2_weight,
    fc2_bias,
    server_of_clip,
):
    bf16 = jnp.bfloat16
    y_at, core_at, zh_at = lax.axis_index("y"), lax.axis_index("core"), lax.axis_index("zh")

    plane = ("zh", "x", "zl", "core")
    w_qkv = lax.all_gather(qkv_weight.reshape(40, 384), plane, axis=0, tiled=True)
    w_out = lax.all_gather(out_weight, ("y",) + plane, axis=0, tiled=True)
    w_one = lax.all_gather(fc1_weight, plane, axis=0, tiled=True)
    w_two = lax.all_gather(fc2_weight, plane, axis=0, tiled=True)

    own = jnp.concatenate([qv_bias[0], qv_bias[1], fc1_bias, fc2_bias, out_bias])
    other = lax.ppermute(own, "zh", [(0, 1), (1, 0)])
    both = jnp.where(zh_at == 0, jnp.stack([own, other]), jnp.stack([other, own]))
    q_bias = both[:, 0:128].reshape(256, 1)
    v_bias = both[:, 128:256].reshape(256, 1)
    one_bias = both[:, 256:896].reshape(1280, 1)
    two_bias = both[:, 896:1056].reshape(320, 1)
    out_pair = both[:, 1056:1216].reshape(320)
    out_all = jnp.zeros((4, 320), jnp.float32)
    out_all = lax.dynamic_update_slice(out_all, out_pair[None], (y_at, 0))
    for step in (1, 2, 3):
        part = lax.ppermute(out_pair, "y", [(at, (at + step) % 4) for at in range(4)])
        out_all = lax.dynamic_update_slice(out_all, part[None], ((y_at - step) % 4, 0))
    out_all = out_all.reshape(1280, 1)

    clip_order = slot_order(server_of_clip)
    source_at = (clip_order % 2) * 16 + clip_order // 2
    source_at = source_at.reshape(16, 2).T.reshape(32)
    pieces = (
        frames_in[0, 0]
        .reshape(2, 160, 4, 160)
        .transpose(0, 3, 2, 1)
        .reshape(32, 10, 640)
    )
    shuffled = exchange(pieces, ("core", "x", "zl"))
    picked = jnp.take(shuffled, source_at, axis=0)
    block = exchange(picked, ("zh", "x", "zl")).reshape(320, 640)
    residual = gather_y(block)

    normed_one = norm_columns(residual, ln1_gain, ln1_bias)
    halves = [dot_rows(w_qkv[at : at + 1280], normed_one) for at in (0, 1280)]
    queries = jnp.concatenate([half[0:128] for half in halves], axis=0)
    queries = ((queries + q_bias) * HDIM ** (-0.5)).astype(bf16)
    keys = jnp.concatenate([half[128:256] for half in halves], axis=0).astype(bf16)
    values = jnp.concatenate([half[256:384] for half in halves], axis=0)
    values = (values + v_bias).astype(bf16)
    mine = jnp.concatenate([keys, values], axis=0)
    theirs = lax.ppermute(mine, "core", [(0, 1), (1, 0)])
    every = jnp.concatenate([mine, theirs], axis=1)
    context = attend(queries, every[:256], every[256:])

    whole_context = gather_y(context)
    attended = (
        residual.astype(jnp.float32) + out_all + dot_rows(w_out, whole_context)
    ).astype(bf16)
    normed_two = norm_columns(attended, ln2_gain, ln2_bias)
    sums = jnp.concatenate([dot_rows(w_one[at : at + 1280], normed_two) for at in (0, 1280)], axis=0)
    hidden = jax.nn.gelu(sums + one_bias, approximate=False).astype(bf16)
    terms = dot_rows(w_two, hidden).astype(bf16).reshape(4, 320, 640)
    arrived = exchange(terms, "y").astype(jnp.float32)
    kept = lax.dynamic_slice(attended, (y_at * 320, 0), (320, 640)).astype(jnp.float32)
    done = (kept + two_bias + jnp.sum(arrived, axis=0)).astype(bf16).reshape(2, 160, 640)

    same = [(j * 2 + k, k * 2 + j) for k in range(2) for j in range(2)]
    cross = [(j * 2 + k, k * 2 + 1 - j) for k in range(2) for j in range(2)]
    first = lax.ppermute(jnp.where(core_at == 0, done[0], done[1]), ("core", "zh"), same)
    second = lax.ppermute(jnp.where(core_at == 0, done[1], done[0]), ("core", "zh"), cross)
    halves = jnp.where(zh_at == 0, jnp.stack([first, second]), jnp.stack([second, first]))
    return halves.reshape(2, 160, 4, 160).transpose(0, 3, 2, 1).reshape(1, 1, 320, 640)


def solution(mesh):
    torus = Mesh(mesh.devices.reshape(4, 4, 2, 4, 2), ("x", "zl", "core", "y", "zh"))
    return jax.shard_map(
        on_device,
        mesh=torus,
        in_specs=(
            P(DP, HEAD, None, None),
            P(),
            P(),
            P(DP, None, HEAD),
            P(None, HEAD),
            P(HEAD + DP, None),
            P(HEAD),
            P(),
            P(),
            P(DP, HEAD),
            P(HEAD),
            P(HEAD + DP, None),
            P(HEAD),
            P(),
        ),
        out_specs=P(DP, HEAD, None, None),
        check_vma=False,
    )
```

```python
import jax
import jax.numpy as jnp
from jax import lax
from jax.sharding import Mesh
from jax.sharding import PartitionSpec as P

HDIM = 64
DP = ("x", "zl", "core")
HEAD = ("y", "zh")
EPS = 1e-05
SWAP = [(0, 1), (1, 0)]


def exchange(value, axes):
    return lax.all_to_all(value, axes, split_axis=0, concat_axis=0, tiled=True)


def gather_y(value):
    copies = jnp.broadcast_to(value[None], (4, *value.shape))
    return exchange(copies, "y").reshape(4 * value.shape[0], value.shape[1])


def ring_gather(value, axes, named, number):
    size, here = lax.axis_size(axes), lax.axis_index(axes)
    out = jnp.zeros((size, *value.shape), value.dtype)
    zeros = (0,) * value.ndim
    out = lax.dynamic_update_slice(out, value[None], (here, *zeros))
    for step in range(1, size):
        pairs = [(number(at), number((at + step) % size)) for at in range(size)]
        part = lax.ppermute(value, named, pairs)
        out = lax.dynamic_update_slice(out, part[None], ((here - step) % size, *zeros))
    return out


def in_thirds(values):
    high = values.astype(jnp.bfloat16)
    rest = values - high.astype(jnp.float32)
    middle = rest.astype(jnp.bfloat16)
    low = (rest - middle.astype(jnp.float32)).astype(jnp.bfloat16)
    return jnp.stack([high, middle, low])


def whole(thirds, axis):
    return jnp.sum(thirds.astype(jnp.float32), axis=axis)


def norm_columns(matrix, gain, shift):
    floats = matrix.astype(jnp.float32)
    center = jnp.mean(floats, axis=0, keepdims=True)
    spread = jnp.mean(jnp.square(floats - center), axis=0, keepdims=True)
    return ((floats - center) * lax.rsqrt(spread + EPS) * gain[:, None] + shift[:, None]).astype(
        jnp.bfloat16
    )


def erf(x):
    x = jnp.clip(x, -3.7439211627767994, 3.7439211627767994)
    square = x * x
    above = jnp.float32(0.00022905065861350646)
    for term in (0.0034082910107109506, 0.050955695062380861, 0.18520832239976145, 1.128379143519084):
        above = above * square + term
    below = jnp.float32(-1.1791602954361697e-7)
    for term in (
        0.000023547966471313185,
        0.0010179625278914885,
        0.014070470171167667,
        0.11098505178285362,
        0.49746925110067538,
        1.0,
    ):
        below = below * square + term
    return x * above / below


def gelu(x):
    return 0.5 * x * (1.0 + erf(x * 0.7071067811865476))


def dot_rows(left, right):
    return lax.dot_general(
        left, right, (((0,), (0,)), ((), ())), preferred_element_type=jnp.float32
    )


def slot_order(server_list):
    clip_count = server_list.shape[0]
    indices = jnp.arange(clip_count, dtype=jnp.int32)
    earlier = (server_list[None, :] < server_list[:, None]) | (
        server_list[None, :] == server_list[:, None]
    ) & (indices[None, :] < indices[:, None])
    slot_of = jnp.sum(earlier.astype(jnp.int32), axis=1)
    return jnp.sum(jnp.where(slot_of[None, :] == indices[:, None], indices[None, :], 0), axis=1)


def attend(queries, key_rows, value_rows):
    outs = []
    for at in range(0, queries.shape[0], HDIM):
        scores = dot_rows(key_rows[at : at + HDIM], queries[at : at + HDIM])
        maxima = jnp.max(scores, axis=0, keepdims=True)
        weights = jnp.exp(scores - maxima)
        probs = (weights / jnp.sum(weights, axis=0, keepdims=True)).astype(jnp.bfloat16)
        outs.append(
            jnp.dot(
                value_rows[at : at + HDIM], probs, preferred_element_type=jnp.float32
            ).astype(jnp.bfloat16)
        )
    return jnp.concatenate(outs, axis=0)


def on_device(
    frames_in,
    ln1_gain,
    ln1_bias,
    qkv_weight,
    qv_bias,
    out_weight,
    out_bias,
    ln2_gain,
    ln2_bias,
    fc1_weight,
    fc1_bias,
    fc2_weight,
    fc2_bias,
    server_of_clip,
):
    bf16 = jnp.bfloat16
    y_at, core_at, zh_at = lax.axis_index("y"), lax.axis_index("core"), lax.axis_index("zh")

    qkv_rows = jnp.concatenate(
        [
            qkv_weight.reshape(40, 384),
            jnp.pad(in_thirds(qv_bias.reshape(256)), ((0, 5), (0, 128))),
        ],
        axis=0,
    )
    qkv_z = ring_gather(qkv_rows, ("zh", "zl"), ("zl", "zh"), lambda at: at % 4 * 2 + at // 4)
    qkv_bias = whole(qkv_z.reshape(2, 4, 48, 384)[:, 0, 40:43, :256], 1)
    q_bias, v_bias = qkv_bias[:, :128].reshape(256, 1), qkv_bias[:, 128:].reshape(256, 1)
    qkv_x = ring_gather(qkv_z[:, :40], "x", "x", lambda at: at).reshape(4, 2, 4, 1, 40, 384)
    qkv_other = lax.ppermute(qkv_x, "core", SWAP)
    qkv_both = jnp.where(
        core_at == 0,
        jnp.concatenate([qkv_x, qkv_other], axis=3),
        jnp.concatenate([qkv_other, qkv_x], axis=3),
    )
    w_qkv = qkv_both.transpose(1, 0, 2, 3, 4, 5).reshape(2, 1280, 384)

    two_own = jnp.where(core_at == 0, fc2_weight[:, :640], fc2_weight[:, 640:])
    two_other = jnp.where(core_at == 0, fc2_weight[:, 640:], fc2_weight[:, :640])
    two_other = lax.ppermute(two_other, "core", SWAP)
    two_rows = jnp.where(
        core_at == 0,
        jnp.concatenate([two_own, two_other], axis=0),
        jnp.concatenate([two_other, two_own], axis=0),
    )
    out_rows = jnp.stack([out_weight[:, :640], out_weight[:, 640:]])
    out_rows = jnp.concatenate(
        [
            out_rows,
            jnp.broadcast_to(
                jnp.pad(in_thirds(out_bias).reshape(480), (0, 160)), (2, 4, 640)
            ),
        ],
        axis=1,
    )
    out_rows = exchange(
        jnp.broadcast_to(out_rows[:, None], (2, 4, 8, 640)).reshape(8, 8, 640), ("core", "y")
    )
    out_rows = out_rows.reshape(2, 4, 8, 640).transpose(1, 0, 2, 3)
    out_biases = whole(out_rows[:, 0, 4, :480].reshape(4, 3, 160), 1)
    out_rows = out_rows[:, :, :4].reshape(32, 640)
    bias_rows = jnp.concatenate(
        [
            in_thirds(fc1_bias),
            jnp.pad(in_thirds(fc2_bias).reshape(1, 480), ((0, 0), (0, 160))),
            jnp.pad(in_thirds(out_biases.reshape(640)), ((0, 1), (0, 0))),
        ],
        axis=0,
    )
    shard = jnp.concatenate([fc1_weight, two_rows, out_rows, bias_rows], axis=0)
    plane = lax.all_gather(shard, ("x", "zh", "zl", "core"), axis=0, tiled=False)
    plane = plane.reshape(4, 2, 4, 2, 120, 640)

    clip_order = slot_order(server_of_clip)
    source_at = clip_order.reshape(4, 4, 2).transpose(0, 2, 1).reshape(32)
    pieces = (
        frames_in[0, 0]
        .reshape(2, 160, 4, 160)
        .transpose(0, 3, 2, 1)
        .reshape(2, 16, 50, 128)
        .transpose(1, 0, 2, 3)
        .reshape(32, 50, 128)
    )
    shuffled = exchange(pieces, ("x", "zl", "core"))
    picked = jnp.take(shuffled, source_at, axis=0)
    block = exchange(picked, ("x", "zh", "zl"))
    block = block.reshape(4, 2, 4, 50, 128).transpose(1, 0, 2, 3, 4).reshape(320, 640)
    residual = gather_y(block)

    normed_one = norm_columns(residual, ln1_gain, ln1_bias)
    halves = [dot_rows(w_qkv[at], normed_one) for at in (0, 1)]
    queries = jnp.concatenate([half[0:128] for half in halves], axis=0)
    queries = ((queries + q_bias) * HDIM ** (-0.5)).astype(bf16)
    keys = jnp.concatenate([half[128:256] for half in halves], axis=0).astype(bf16)
    values = jnp.concatenate([half[256:384] for half in halves], axis=0)
    values = (values + v_bias).astype(bf16)
    mine = jnp.concatenate([keys, values], axis=0)
    theirs = lax.ppermute(mine, "core", SWAP)
    every = jnp.concatenate([mine, theirs], axis=1)
    context = attend(queries, every[:256], every[256:])

    whole_context = gather_y(context)
    w_one = plane[:, :, :, :, 0:40].transpose(1, 0, 2, 3, 4, 5).reshape(2, 1280, 640)
    w_two = plane[:, :, :, :, 40:80].transpose(3, 1, 0, 2, 4, 5).reshape(2, 1280, 640)
    w_out = (
        plane[:, :, :, :, 80:112]
        .reshape(4, 2, 4, 2, 4, 8, 640)
        .transpose(3, 4, 1, 0, 2, 5, 6)
        .reshape(2, 1024, 640)
    )
    out_all = whole(plane[0, :, 0, 0, 116:119], 1).reshape(2, 4, 160)
    out_all = out_all.transpose(1, 0, 2).reshape(1280, 1)
    one_bias = whole(plane[0, :, 0, 0, 112:115], 1).reshape(1280, 1)
    two_bias = whole(plane[0, :, 0, 0, 115, :480].reshape(2, 3, 160), 1).reshape(320, 1)

    attended = (
        residual.astype(jnp.float32)
        + out_all
        + jnp.concatenate([dot_rows(half, whole_context) for half in w_out], axis=0)
    ).astype(bf16)
    normed_two = norm_columns(attended, ln2_gain, ln2_bias)
    sums = jnp.concatenate([dot_rows(w_one[at], normed_two) for at in (0, 1)], axis=0)
    hidden = gelu(sums + one_bias).astype(bf16)
    hidden = lax.optimization_barrier(hidden)
    terms = jnp.concatenate([dot_rows(half, hidden) for half in w_two], axis=0)
    terms = terms.astype(bf16).reshape(4, 320, 640)
    arrived = exchange(terms, "y").astype(jnp.float32)
    kept = lax.dynamic_slice(attended, (y_at * 320, 0), (320, 640)).astype(jnp.float32)
    done = (kept + two_bias + jnp.sum(arrived, axis=0)).astype(bf16).reshape(2, 160, 640)

    same = [(j * 2 + k, k * 2 + j) for k in range(2) for j in range(2)]
    cross = [(j * 2 + k, k * 2 + 1 - j) for k in range(2) for j in range(2)]
    first = lax.ppermute(jnp.where(core_at == 0, done[0], done[1]), ("core", "zh"), same)
    second = lax.ppermute(jnp.where(core_at == 0, done[1], done[0]), ("core", "zh"), cross)
    halves = jnp.where(zh_at == 0, jnp.stack([first, second]), jnp.stack([second, first]))
    return halves.reshape(2, 160, 4, 160).transpose(0, 3, 2, 1).reshape(1, 1, 320, 640)


def solution(mesh):
    torus = Mesh(mesh.devices.reshape(4, 4, 2, 4, 2), ("x", "zl", "core", "y", "zh"))
    return jax.shard_map(
        on_device,
        mesh=torus,
        in_specs=(
            P(DP, HEAD, None, None),
            P(),
            P(),
            P(DP, None, HEAD),
            P(None, HEAD),
            P(HEAD + DP, None),
            P(HEAD),
            P(),
            P(),
            P(DP, HEAD),
            P(HEAD),
            P(HEAD + DP, None),
            P(HEAD),
            P(),
        ),
        out_specs=P(DP, HEAD, None, None),
        check_vma=False,
    )
```

```python
import functools

import jax
import jax.numpy as jnp
from jax import lax
from jax.experimental import pallas as pl
from jax.experimental.pallas import tpu as pltpu
from jax.sharding import Mesh
from jax.sharding import PartitionSpec as P


HDIM = 64
DP = ("x", "zl", "core")
HEAD = ("y", "zh")
EPS = 1e-05
SWAP = [(0, 1), (1, 0)]


def exchange(value, axes):
    return lax.all_to_all(value, axes, split_axis=0, concat_axis=0, tiled=True)


def gather_y(value):
    copies = jnp.broadcast_to(value[None], (4, *value.shape))
    return exchange(copies, "y").reshape(4 * value.shape[0], value.shape[1])


def ring_gather(value, axis):
    size, here = lax.axis_size(axis), lax.axis_index(axis)
    out = jnp.zeros((size, *value.shape), value.dtype)
    zeros = (0,) * value.ndim
    out = lax.dynamic_update_slice(out, value[None], (here, *zeros))
    for step in range(1, size):
        part = lax.ppermute(value, axis, [(at, (at + step) % size) for at in range(size)])
        out = lax.dynamic_update_slice(out, part[None], ((here - step) % size, *zeros))
    return out


def doubling_gather(value, bits):
    for depth, (axis, bit) in enumerate(bits):
        size = lax.axis_size(axis)
        other = lax.ppermute(value, axis, [(at, at ^ (1 << bit)) for at in range(size)])
        high = (lax.axis_index(axis) >> bit) & 1
        value = jnp.where(
            high == 0,
            jnp.stack([value, other], axis=depth),
            jnp.stack([other, value], axis=depth),
        )
    return value


def in_thirds(values):
    high = values.astype(jnp.bfloat16)
    rest = values - high.astype(jnp.float32)
    middle = rest.astype(jnp.bfloat16)
    low = (rest - middle.astype(jnp.float32)).astype(jnp.bfloat16)
    return jnp.stack([high, middle, low])


def whole(thirds, axis):
    return jnp.sum(thirds.astype(jnp.float32), axis=axis)


def norm_rows(floats, gain_ref, shift_ref):
    floats = floats - jnp.mean(floats, axis=1, keepdims=True)
    spread = jnp.mean(jnp.square(floats), axis=1, keepdims=True)
    normed = floats * lax.rsqrt(spread + EPS) * gain_ref[...] + shift_ref[...]
    return normed.astype(jnp.bfloat16)


def erf(x):
    x = jnp.clip(x, -3.7439211627767994, 3.7439211627767994)
    square = x * x
    above = jnp.float32(0.00022905065861350646)
    for term in (0.0034082910107109506, 0.050955695062380861, 0.18520832239976145, 1.128379143519084):
        above = above * square + term
    below = jnp.float32(-1.1791602954361697e-7)
    for term in (
        0.000023547966471313185,
        0.0010179625278914885,
        0.014070470171167667,
        0.11098505178285362,
        0.49746925110067538,
        1.0,
    ):
        below = below * square + term
    return x * above / below


def gelu(x):
    return 0.5 * x * (1.0 + erf(x * 0.7071067811865476))


def dot_rows(left, right):
    return lax.dot_general(
        left, right, (((0,), (0,)), ((), ())), preferred_element_type=jnp.float32
    )


def slot_order(server_list):
    clip_count = server_list.shape[0]
    indices = jnp.arange(clip_count, dtype=jnp.int32)
    earlier = (server_list[None, :] < server_list[:, None]) | (
        server_list[None, :] == server_list[:, None]
    ) & (indices[None, :] < indices[:, None])
    slot_of = jnp.sum(earlier.astype(jnp.int32), axis=1)
    return jnp.sum(jnp.where(slot_of[None, :] == indices[:, None], indices[None, :], 0), axis=1)


def in_hbm(value):
    return pltpu.with_memory_space_constraint(value, pltpu.HBM)


def assemble_kernel(one_ref, first_ref, second_ref, out_ref, bias_ref, shard_ref):
    parts = [one_ref[...], first_ref[0:20, :], second_ref[0:20, :]]
    parts += [out_ref[y, 0:8, :] for y in range(4)]
    parts += [bias_ref[...]] + [out_ref[y, 8:9, :] for y in range(4)]
    rows = jnp.concatenate([part.astype(jnp.float32) for part in parts], axis=0)
    shard_ref[...] = rows.astype(jnp.bfloat16)


def assembled(*arrays):
    vmem = pl.BlockSpec(memory_space=pltpu.VMEM)
    return pl.pallas_call(
        assemble_kernel,
        in_specs=[vmem] * 5,
        out_specs=vmem,
        out_shape=jax.ShapeDtypeStruct((120, 640), jnp.bfloat16),
        compiler_params=pltpu.CompilerParams(vmem_limit_bytes=4 << 20),
        cost_estimate=pl.CostEstimate(flops=1 << 20, transcendentals=0, bytes_accessed=1 << 19),
    )(*arrays)


def attend_pack_kernel(low, q_ref, mine_ref, theirs_ref, plane_ref, context_ref, wo_to, w1_to,
                       w2_to, wo_ref, w1_ref, w2_ref, sems):
    def start(at, carry):
        x, zh, zl, core = at // 16, at // 8 % 2, at // 2 % 4, at % 2
        block = plane_ref.at[x, zh, zl, core]
        group = x * 4 + zl
        pltpu.make_async_copy(
            block.at[pl.ds(10, 4)], wo_ref.at[core, :, zh * 16 + group], sems.at[0]
        ).start()
        pltpu.make_async_copy(
            block.at[pl.ds(0, 5)], w1_ref.at[zh, pl.ds((group * 2 + core) * 5, 5)], sems.at[1]
        ).start()
        pltpu.make_async_copy(
            block.at[pl.ds(5, 5)], w2_ref.at[core, pl.ds((zh * 16 + group) * 5, 5)], sems.at[2]
        ).start()
        return carry

    lax.fori_loop(0, 64, start, 0)
    attend_kernel(low, q_ref, mine_ref, theirs_ref, context_ref)
    outward = []
    for at, (ref, target) in enumerate(((wo_ref, wo_to), (w1_ref, w1_to), (w2_ref, w2_to))):
        pltpu.make_async_copy(target, ref, sems.at[at]).wait()
        outward.append(pltpu.make_async_copy(ref, target, sems.at[3 + at]))
        outward[-1].start()
    for copy in outward:
        copy.wait()


def attend_packed(low, width, plane, *arrays):
    shapes = ((2, 4, 32, 8, 640), (2, 160, 8, 640), (2, 160, 8, 640))
    vmem, hbm = pl.BlockSpec(memory_space=pltpu.VMEM), pl.BlockSpec(memory_space=pltpu.HBM)
    context, *weights = pl.pallas_call(
        functools.partial(attend_pack_kernel, low),
        in_specs=[vmem] * 3 + [hbm],
        out_specs=[vmem] + [hbm] * 3,
        out_shape=[jax.ShapeDtypeStruct((256, width), jnp.bfloat16)]
        + [pltpu.HBM(shape, jnp.bfloat16) for shape in shapes],
        scratch_shapes=[pltpu.VMEM(shape, jnp.bfloat16) for shape in shapes]
        + [pltpu.SemaphoreType.DMA((6,))],
        compiler_params=pltpu.CompilerParams(vmem_limit_bytes=22 << 20),
        cost_estimate=pl.CostEstimate(flops=1 << 30, transcendentals=0, bytes_accessed=20 << 20),
    )(*arrays, in_hbm(plane.reshape(4, 2, 4, 2, 15, 8, 640)))
    return context, [weight.reshape(2, -1, 640) for weight in weights]


def qkv_kernel(x_ref, w_ref, bias_ref, gain_ref, shift_ref, q_ref, kv_ref, n_ref):
    n_ref[...] = norm_rows(jnp.transpose(x_ref[...]).astype(jnp.float32), gain_ref, shift_ref)

    def one_half(half, carry):
        projected = jnp.dot(n_ref[...], w_ref[half], preferred_element_type=jnp.float32)
        projected = projected + bias_ref[half]
        queries = (projected[:, 0:128] * HDIM ** (-0.5)).astype(jnp.bfloat16)
        rows = pl.ds(pl.multiple_of(128 * half, 128), 128)
        q_ref[rows, :] = jnp.transpose(queries)
        kv_ref[rows, :] = jnp.transpose(projected[:, 128:256].astype(jnp.bfloat16))
        rows = pl.ds(pl.multiple_of(256 + 128 * half, 128), 128)
        kv_ref[rows, :] = jnp.transpose(projected[:, 256:384].astype(jnp.bfloat16))
        return carry

    lax.fori_loop(0, 2, one_half, 0)


def qkv_rows_of(*arrays):
    vmem = pl.BlockSpec(memory_space=pltpu.VMEM)
    return pl.pallas_call(
        qkv_kernel,
        in_specs=[vmem] * 5,
        out_specs=[vmem, vmem],
        out_shape=[
            jax.ShapeDtypeStruct((256, 640), jnp.bfloat16),
            jax.ShapeDtypeStruct((512, 640), jnp.bfloat16),
        ],
        scratch_shapes=[pltpu.VMEM((640, 1280), jnp.bfloat16)],
        compiler_params=pltpu.CompilerParams(vmem_limit_bytes=20 << 20),
        cost_estimate=pl.CostEstimate(
            flops=2 * 640 * 1280 * 768, transcendentals=0, bytes_accessed=4 << 20
        ),
    )(*arrays)


def attend_kernel(low, q_ref, mine_ref, theirs_ref, context_ref):
    width = context_ref.shape[1]

    def one_head(head, carry):
        at = pl.multiple_of(head * HDIM, HDIM)
        queries = q_ref[pl.ds(at, HDIM), low : low + width]
        scores = [dot_rows(ref[pl.ds(at, HDIM), :], queries) for ref in (mine_ref, theirs_ref)]
        maxima = jnp.maximum(*(jnp.max(part, axis=0, keepdims=True) for part in scores))
        weights = [jnp.exp(part - maxima) for part in scores]
        total = sum(jnp.sum(part, axis=0, keepdims=True) for part in weights)
        mixed = sum(
            jnp.dot(
                ref[pl.ds(pl.multiple_of(256 + at, HDIM), HDIM), :],
                part.astype(jnp.bfloat16),
                preferred_element_type=jnp.float32,
            )
            for ref, part in zip((mine_ref, theirs_ref), weights)
        )
        context_ref[pl.ds(at, HDIM), :] = (mixed / total).astype(jnp.bfloat16)
        return carry

    lax.fori_loop(0, 4, one_head, 0)


def attend(low, width, *arrays):
    vmem = pl.BlockSpec(memory_space=pltpu.VMEM)
    return pl.pallas_call(
        functools.partial(attend_kernel, low),
        in_specs=[vmem] * 3,
        out_specs=vmem,
        out_shape=jax.ShapeDtypeStruct((256, width), jnp.bfloat16),
        compiler_params=pltpu.CompilerParams(vmem_limit_bytes=14 << 20),
        cost_estimate=pl.CostEstimate(
            flops=4 * 1280 * width * 256, transcendentals=1280 * width * 4, bytes_accessed=2 << 20
        ),
    )(*arrays)


def mlp_kernel(low, at_ref, x_ref, c_ref, wo_from, w1_from, w2_from, ob_ref, gain_ref, shift_ref,
               b1_ref, kept_ref, terms_ref, att_ref, p_ref, n_ref, h_ref, wo_ref, w1_ref, w2_ref,
               sems):
    copies = [
        pltpu.make_async_copy(source, ref, sems.at[at])
        for at, (source, ref) in enumerate(
            ((wo_from, wo_ref), (w1_from, w1_ref), (w2_from, w2_ref))
        )
    ]
    for copy in copies:
        copy.start()
    width = c_ref.shape[1]

    def project(half, carry):
        p_ref[half] = dot_rows(c_ref[...], wo_ref[half])
        return carry

    def up(half, carry):
        sums = jnp.dot(n_ref[...], w1_ref[half], preferred_element_type=jnp.float32)
        h_ref[half] = gelu(sums + b1_ref[half]).astype(jnp.bfloat16)
        return carry

    def down(half, carry):
        terms = sum(
            jnp.dot(
                h_ref[part],
                w2_ref[half, 640 * part : 640 * part + 640, :],
                preferred_element_type=jnp.float32,
            )
            for part in (0, 1)
        )
        rows = pl.ds(pl.multiple_of(half * 640, 640), 640)
        terms_ref[rows, :] = jnp.transpose(terms.astype(jnp.bfloat16))
        return carry

    copies[0].wait()
    lax.fori_loop(0, 2, project, 0)
    residual = jnp.transpose(x_ref[:, low : low + width]).astype(jnp.float32)
    projected = jnp.concatenate([p_ref[0], p_ref[1]], axis=1)
    attended = (residual + ob_ref[...] + projected).astype(jnp.bfloat16)
    att_ref[...] = jnp.transpose(attended)
    kept_ref[...] = att_ref[pl.ds(pl.multiple_of(at_ref[0] * 320, 320), 320), :]
    n_ref[...] = norm_rows(attended.astype(jnp.float32), gain_ref, shift_ref)
    copies[1].wait()
    lax.fori_loop(0, 2, up, 0)
    copies[2].wait()
    lax.fori_loop(0, 2, down, 0)


def mlp_chunk(low, block_at, residual, context, *weights):
    width = context.shape[1]
    spaces = [pl.BlockSpec(memory_space=pltpu.SMEM)]
    spaces += [pl.BlockSpec(memory_space=pltpu.VMEM)] * 2
    spaces += [pl.BlockSpec(memory_space=pltpu.HBM)] * 3
    spaces += [pl.BlockSpec(memory_space=pltpu.VMEM)] * (len(weights) - 3)
    return pl.pallas_call(
        functools.partial(mlp_kernel, low),
        in_specs=spaces,
        out_specs=[pl.BlockSpec(memory_space=pltpu.VMEM)] * 2,
        out_shape=[
            jax.ShapeDtypeStruct((320, width), jnp.bfloat16),
            jax.ShapeDtypeStruct((1280, width), jnp.bfloat16),
        ],
        scratch_shapes=[
            pltpu.VMEM((1280, width), jnp.bfloat16),
            pltpu.VMEM((2, width, 640), jnp.float32),
            pltpu.VMEM((width, 1280), jnp.bfloat16),
            pltpu.VMEM((2, width, 640), jnp.bfloat16),
        ]
        + [pltpu.VMEM(weight.shape, jnp.bfloat16) for weight in weights[:3]]
        + [pltpu.SemaphoreType.DMA((3,))],
        compiler_params=pltpu.CompilerParams(vmem_limit_bytes=28 << 20),
        cost_estimate=pl.CostEstimate(
            flops=2 * width * 1280 * (1024 + 2560), transcendentals=0, bytes_accessed=12 << 20
        ),
    )(block_at, residual, context, *(in_hbm(weight) for weight in weights[:3]), *weights[3:])


def layer(
    frames_in,
    ln1_gain,
    ln1_bias,
    qkv_weight,
    qv_bias,
    out_weight,
    out_bias,
    ln2_gain,
    ln2_bias,
    fc1_weight,
    fc1_bias,
    fc2_weight,
    fc2_bias,
    server_of_clip,
):
    bf16 = jnp.bfloat16
    y_at, core_at, zh_at = lax.axis_index("y"), lax.axis_index("core"), lax.axis_index("zh")

    clip_order = slot_order(server_of_clip)
    source_at = clip_order.reshape(4, 4, 2).transpose(0, 2, 1).reshape(32)
    pieces = (
        frames_in[0, 0]
        .reshape(2, 160, 4, 160)
        .transpose(0, 3, 2, 1)
        .reshape(2, 16, 50, 128)
        .transpose(1, 0, 2, 3)
        .reshape(32, 50, 128)
    )
    shuffled = exchange(pieces, ("x", "zl", "core"))
    picked = shuffled.at[source_at].get(mode="promise_in_bounds")
    block = exchange(picked, ("x", "zh", "zl"))
    block = block.reshape(4, 2, 4, 50, 128).transpose(1, 0, 2, 3, 4).reshape(320, 640)
    rows = jnp.concatenate([fc2_weight, out_weight], axis=0)
    rows_own = jnp.where(core_at == 0, rows[:, :640], rows[:, 640:])
    rows_other = jnp.where(core_at == 0, rows[:, 640:], rows[:, :640])
    rows_other = lax.ppermute(rows_other, "core", SWAP)
    first = jnp.where(core_at == 0, rows_own, rows_other)
    second = jnp.where(core_at == 0, rows_other, rows_own)
    out_rows = jnp.concatenate(
        [first[20:], second[20:], jnp.pad(in_thirds(out_bias).reshape(1, 480), ((0, 7), (0, 160)))],
        axis=0,
    )
    out_rows = doubling_gather(out_rows, (("y", 1), ("y", 0))).reshape(4, 16, 640)
    bias_rows = jnp.concatenate(
        [in_thirds(fc1_bias), jnp.pad(in_thirds(fc2_bias).reshape(1, 480), ((0, 0), (0, 160)))],
        axis=0,
    )
    shard = assembled(fc1_weight, first, second, out_rows, bias_rows)
    plane = lax.all_gather(shard, ("x", "zh", "zl", "core"), axis=0, tiled=False)
    plane = plane.reshape(4, 2, 4, 2, 120, 640)

    qkv_rows = jnp.concatenate(
        [qkv_weight.reshape(40, 384), jnp.pad(in_thirds(qv_bias.reshape(256)), ((0, 5), (0, 128)))],
        axis=0,
    )
    qkv_z = doubling_gather(qkv_rows, (("zh", 0), ("zl", 1), ("zl", 0)))
    qkv_z = qkv_z.reshape(8, 48, 384)
    qkv_bias = whole(qkv_z.reshape(2, 4, 48, 384)[:, 0, 40:43, :256], 1)
    qkv_bias = jnp.concatenate(
        [qkv_bias[:, :128], jnp.zeros((2, 128), jnp.float32), qkv_bias[:, 128:]], axis=1
    ).reshape(2, 1, 384)
    qkv_x = ring_gather(qkv_z[:, :40], "x").reshape(4, 2, 4, 1, 40, 384)
    qkv_other = lax.ppermute(qkv_x, "core", SWAP)
    qkv_both = jnp.where(
        core_at == 0,
        jnp.concatenate([qkv_x, qkv_other], axis=3),
        jnp.concatenate([qkv_other, qkv_x], axis=3),
    )
    w_qkv = qkv_both.transpose(1, 0, 2, 3, 4, 5).reshape(2, 1280, 384)

    residual = gather_y(block)

    queries, mine = qkv_rows_of(
        residual, w_qkv, qkv_bias, ln1_gain.reshape(1, 1280), ln1_bias.reshape(1, 1280)
    )
    theirs = lax.ppermute(mine, "core", SWAP)
    chunks = ((0, 384), (384, 640))
    contexts = []
    for at, (low, high) in enumerate(chunks):
        if at == 0:
            part = attend(low, high - low, queries, mine, theirs)
        else:
            part, packed = attend_packed(low, high - low, plane, queries, mine, theirs)
        contexts.append(gather_y(part))

    w_out, w_one, w_two = packed
    out_all = whole(plane[0, :, 0, 0, 116:120, :480].reshape(2, 4, 3, 160), 2)
    out_all = out_all.transpose(1, 0, 2).reshape(1280, 1)
    one_bias = whole(plane[0, :, 0, 0, 112:115], 1).reshape(1280, 1)
    two_bias = whole(plane[0, :, 0, 0, 115, :480].reshape(2, 3, 160), 1).reshape(320, 1)

    out_row, one_row = out_all.reshape(1, 1280), one_bias.reshape(2, 1, 640)
    gain_row, shift_row = ln2_gain.reshape(1, 1280), ln2_bias.reshape(1, 1280)
    block_at = y_at.astype(jnp.int32).reshape(1)
    ends = []
    for at, (low, high) in enumerate(chunks):
        width = high - low
        kept, terms = mlp_chunk(
            low, block_at, residual, contexts[at], w_out, w_one, w_two,
            out_row, gain_row, shift_row, one_row,
        )
        terms = terms.reshape(4, 320, width)
        arrived = exchange(terms, "y").astype(jnp.float32)
        done = (kept.astype(jnp.float32) + two_bias + jnp.sum(arrived, axis=0)).astype(bf16).reshape(2, 160, width)

        same = [(j * 2 + k, k * 2 + j) for k in range(2) for j in range(2)]
        cross = [(j * 2 + k, k * 2 + 1 - j) for k in range(2) for j in range(2)]
        first = lax.ppermute(jnp.where(core_at == 0, done[0], done[1]), ("core", "zh"), same)
        second = lax.ppermute(jnp.where(core_at == 0, done[1], done[0]), ("core", "zh"), cross)
        ends.append(jnp.where(zh_at == 0, jnp.stack([first, second]), jnp.stack([second, first])))
    halves = jnp.concatenate(ends, axis=2)
    return halves.reshape(2, 160, 4, 160).transpose(0, 3, 2, 1).reshape(1, 1, 320, 640)


def solution(mesh):
    torus = Mesh(mesh.devices.reshape(4, 4, 2, 4, 2), ("x", "zl", "core", "y", "zh"))
    return jax.shard_map(
        layer,
        mesh=torus,
        in_specs=(
            P(DP, HEAD, None, None),
            P(),
            P(),
            P(DP, None, HEAD),
            P(None, HEAD),
            P(HEAD + DP, None),
            P(HEAD),
            P(),
            P(),
            P(DP, HEAD),
            P(HEAD),
            P(HEAD + DP, None),
            P(HEAD),
            P(),
        ),
        out_specs=P(DP, HEAD, None, None),
        check_vma=False,
    )
```
